128 devices in a mesh: dp: 32 (over x, z, core), tensor: 4 (over y).
Axes of the slice: x: 4, y: 4, z: 4, core: 2. Of those that a mesh axis runs over, the one named last changes fastest.
Arguments:
- tokens: bfloat16 [2, 2048, 4096], P(None, 'dp', 'tensor'), may hold values from -6 to 6
- routes: int32 [2, 2048, 2], P(None, 'dp'), may hold values from 0 to 7, all different within a row; in each aligned block of 64 rows (0 to 63, 64 to 127, ..., all dimensions but the last counted through in order) at most 20 rows name the same one
- probs: float32 [2, 2048, 8], P(None, 'dp'), may hold values from 0 to 1, as said below
- w_gate: bfloat16 [32, 4096, 3584], P('dp', None, 'tensor'), may hold values from -0.09375 to 0.09375
- w_up: bfloat16 [32, 4096, 3584], P('dp', None, 'tensor'), may hold values from -0.09375 to 0.09375
- w_down: bfloat16 [32, 3584, 4096], P('dp', 'tensor'), may hold values from -0.046875 to 0.046875
Outputs:
- mixed: bfloat16 [2, 2048, 4096], P(None, 'dp', 'tensor')
- aux_loss: float32 [2, 8], replicated
The draws below stay inside these ranges and needn't reach their ends.
Inputs may be any that keep to these rules, and one draw needn't show every extreme that they name: `routes`: in each aligned block of 64 rows (the rows of one index of dp in one micro-batch) no expert is named in more than 20 entries; the 2 experts of a row differ. `probs`: each row is positive and sums to one.
All inputs are finite; a program needn't handle non-finite values.
Results may differ from the reference program's by a relative error of at most 0.012.
Values may be sent and summed in bfloat16 or wider, within the bound.
A program may use at most 128 MiB of HBM per device.

```python
import math
import jax
import jax.numpy as jnp
import numpy as np
from jax import lax

D = 4096
FF = 14336
EXPERTS = 8
TOP = 2
MICRO = 2
MB_DEV = 64
CAP = 20
MB_TOK = 2048
BLOCKS = 32
FF_BLK = 3584
N_DP = 32
N_TENSOR = 4


def draw_probs(key, part):
    first, second, third = jax.random.split(jax.random.fold_in(key, 71), 3)
    group_count = MB_TOK // MB_DEV
    group = jnp.arange(MB_TOK, dtype=jnp.int32) // MB_DEV
    along = group.astype(jnp.float32) / max(group_count - 1, 1)
    micro_ids = jnp.arange(MICRO, dtype=jnp.int32)
    expert_ids = jnp.arange(EXPERTS, dtype=jnp.int32)
    leading = (micro_ids * 3 + 1) % EXPERTS
    marked = (leading[:, None, None] == expert_ids[None, None, :]).astype(jnp.float32)
    rotating = (group[None, :] + micro_ids[:, None] * 5 + 2) % EXPERTS
    second_mark = (rotating[:, :, None] == expert_ids[None, None, :]).astype(jnp.float32)
    common = 0.5 * jax.random.normal(third, (1, 1, EXPERTS), jnp.float32)
    noise = jax.random.normal(first, (MICRO, MB_TOK, EXPERTS), jnp.float32)
    strength = 1.0 + 4.0 * along
    row_scale = jnp.exp(jax.random.uniform(second, (MICRO, MB_TOK, 1), jnp.float32, 0.0, jnp.log(2.0)))
    logits = noise * row_scale * 0.5 + strength[None, :, None] * marked + second_mark + common
    return jax.nn.softmax(logits, axis=-1).astype(jnp.float32)


def shard_levels(own_key, extent, shards, least, high):
    def one(axis_at, blocks):
        steps = jax.random.uniform(jax.random.fold_in(jax.random.fold_in(own_key, 6), axis_at), (blocks,), jnp.float32, least / len(shards), high / len(shards))
        return jnp.repeat(jnp.exp(steps), extent[axis_at] // blocks).reshape((-1,) + (1,) * (len(extent) - axis_at - 1))

    factor_of = one(*shards[0])
    for cut in shards[1:]:
        factor_of = factor_of * one(*cut)
    return factor_of


def deal_out(own_key, own, number, rows, amount, top, limit, slope):
    sequence = jax.random.permutation(own_key, amount)
    crowded, ordinary = load_shares(amount, rows * top, limit, slope, True), load_shares(amount, rows * top, limit, slope, False)
    places = jnp.arange(amount)

    def named(sizes, rotation):
        used = int((sizes > 0).sum())
        fixed = max(1, used // 4)
        moved = fixed + (places - fixed + rotation * (used - fixed)) % max(1, amount - fixed)
        return jnp.zeros((amount,), jnp.int32).at[sequence[jnp.where(places < fixed, places, moved)]].set(jnp.asarray(sizes, jnp.int32))

    sizes = jnp.where(number % 4 == 0, named(crowded, number // 4), named(ordinary, number - number // 4 - 1))
    mixed = jax.random.permutation(jax.random.fold_in(own, 3), amount)
    giver, receiver = mixed[0:amount // 2 * 2:2], mixed[1:amount // 2 * 2:2]
    room = jnp.minimum(sizes[giver] - 1, limit - sizes[receiver]) // 2
    room = jnp.where((giver == sequence[0]) | (receiver == sequence[0]) | (sizes[receiver] == 0), 0, jnp.maximum(room, 0))
    moved = jax.random.randint(jax.random.fold_in(own, 4), (amount // 2,), 0, 1 << 20) % (room + 1)
    sizes = sizes.at[giver].add(-moved).at[receiver].add(moved)
    items = jnp.searchsorted(jnp.cumsum(sizes), jnp.arange(rows * top), side="right").astype(jnp.int32)
    listing = items.reshape(top, rows).T
    listing = listing[jax.random.permutation(jax.random.fold_in(own, 1), rows)]
    rotation = jax.random.randint(jax.random.fold_in(own, 2), (rows, 1), 0, top)
    return jnp.take_along_axis(listing, (jnp.arange(top)[None, :] + rotation) % top, axis=1)


def load_shares(amount, total, reach, lean, full):
    portions = [(1 << 20) // math.isqrt(rank ** lean) + 1 for rank in range(1, amount + 1)]
    largest = reach if full else min(reach, max(-(-total // amount), total * portions[0] // sum(portions)))
    least = 1 if total - largest >= amount - 1 else 0
    given, rest = [largest] + [least] * (amount - 1), total - largest - least * (amount - 1)
    while rest > 0:
        candidates = [i for i in range(1, amount) if given[i] < largest] or [i for i in range(1, amount) if given[i] < reach]
        whole, remaining = sum([portions[i] for i in candidates]), rest
        for i in candidates:
            addition = min(reach - given[i], max(1, remaining * portions[i] // whole), rest)
            given[i] = given[i] + addition
            rest = rest - addition
    return np.array(given)


def bell_draw(own_key, shape, deviation, reach, cuts=(), kind=jnp.bfloat16):
    loudness = shard_levels(own_key, shape, cuts, -0.22, 0.18) if cuts else 1.0
    values = jax.random.normal(own_key, shape, jnp.float32) * deviation * loudness
    return jnp.minimum(jnp.maximum(values, -reach), reach).astype(kind)


def setup_inputs(seed: int = 0) -> dict:
    key_list = jax.random.split(jax.random.key(seed), 7)
    tokens = bell_draw(key_list[0], (MICRO, MB_TOK, D), 1.0, 6.0, ((1, 32), (2, 4)))
    routes_keys = jax.random.split(jax.random.fold_in(key_list[1], 1), MICRO * MB_TOK // MB_DEV)
    routes_turns = jax.random.permutation(jax.random.fold_in(key_list[1], 3), MICRO * MB_TOK // MB_DEV)
    routes = jax.vmap(lambda own, number: deal_out(jax.random.fold_in(key_list[1], 2), own, number, MB_DEV, EXPERTS, TOP, CAP, 1))(routes_keys, routes_turns).reshape((MICRO, MB_TOK, TOP))
    probs = draw_probs(jax.random.fold_in(key_list[6], 71), 0)
    w_gate = bell_draw(key_list[3], (BLOCKS, D, FF_BLK), D ** -0.5, 0.09375, ((0, 32), (2, 4)))
    w_up = bell_draw(key_list[4], (BLOCKS, D, FF_BLK), D ** -0.5, 0.09375, ((0, 32), (2, 4)))
    w_down = bell_draw(key_list[5], (BLOCKS, FF_BLK, D), FF ** -0.5, 0.046875, ((0, 32), (1, 4)))
    return {"tokens": tokens, "routes": routes, "probs": probs, "w_gate": w_gate, "w_up": w_up, "w_down": w_down}


def slot_tables(route, prob):
    rows_count = route.shape[0]
    experts = prob.shape[-1]
    capacity = CAP
    flat = route.reshape(-1)
    onehot = (flat[:, None] == jnp.arange(experts, dtype=jnp.int32)[None, :]).astype(jnp.int32)
    before = jnp.cumsum(onehot, axis=0) - onehot
    place = jnp.sum(before * onehot, axis=1)
    slot = flat * capacity + place
    picked = jnp.take_along_axis(prob, route, axis=1)
    weights = picked / jnp.sum(picked, axis=1, keepdims=True)
    grid = (slot[:, None] == jnp.arange(experts * capacity, dtype=jnp.int32)[None, :]).astype(jnp.float32)
    grid = grid.reshape(rows_count, route.shape[1], experts * capacity)
    dispatch = jnp.sum(grid, axis=1).T.astype(jnp.bfloat16)
    combine = jnp.sum(grid * weights[:, :, None], axis=1)
    counts = jnp.sum(onehot, axis=0).astype(jnp.float32)
    return dispatch, combine, counts


def reference(tokens, routes, probs, w_gate, w_up, w_down):
    per_expert = N_DP // EXPERTS
    quarter = FF // (per_expert * N_TENSOR)
    loss_terms = []
    outputs = []
    for micro_index in range(MICRO):
        tok_groups = tokens[micro_index].reshape(N_DP, MB_DEV, D)
        route_groups = routes[micro_index].reshape(N_DP, MB_DEV, TOP)
        prob_groups = probs[micro_index].reshape(N_DP, MB_DEV, EXPERTS)
        dispatch, combine, counts = jax.vmap(slot_tables)(route_groups, prob_groups)
        slots = jnp.einsum("psr,prd->psd", dispatch.astype(jnp.float32), tok_groups.astype(jnp.float32)).astype(jnp.bfloat16)
        expert_rows = slots.reshape(N_DP, EXPERTS, CAP, D).transpose(1, 0, 2, 3).reshape(EXPERTS, N_DP * CAP, D)

        def one_expert(args):
            expert_id, rows_in = args

            def add_block(block, total):
                sub = (block // N_TENSOR).astype(jnp.int32)
                column = ((block % N_TENSOR) * quarter).astype(jnp.int32)
                index = (expert_id * per_expert + sub).astype(jnp.int32)
                zero = jnp.int32(0)
                gate_block = lax.dynamic_slice(w_gate, (index, zero, column), (1, D, quarter))[0]
                up_block = lax.dynamic_slice(w_up, (index, zero, column), (1, D, quarter))[0]
                down_block = lax.dynamic_slice(w_down, (index, column, zero), (1, quarter, D))[0]
                gate = jnp.dot(rows_in, gate_block, preferred_element_type=jnp.float32)
                up = jnp.dot(rows_in, up_block, preferred_element_type=jnp.float32)
                hidden = (jax.nn.silu(gate) * up).astype(jnp.bfloat16)
                part = jnp.dot(hidden, down_block, preferred_element_type=jnp.float32).astype(jnp.bfloat16)
                part = lax.optimization_barrier(part)
                return total + part.astype(jnp.float32)

            start = jnp.zeros((N_DP * CAP, D), jnp.float32)
            return lax.fori_loop(0, per_expert * N_TENSOR, add_block, start)

        sums = lax.map(one_expert, (jnp.arange(EXPERTS, dtype=jnp.int32), expert_rows))
        sums = sums.reshape(EXPERTS, N_DP, CAP, D).transpose(1, 0, 2, 3).reshape(N_DP, EXPERTS * CAP, D)
        mixed = jnp.einsum("prs,psd->prd", combine, sums, precision=lax.Precision.HIGHEST)
        outputs.append(mixed.reshape(MB_TOK, D).astype(jnp.bfloat16))
        count_all = jnp.sum(counts, axis=0)
        prob_all = jnp.sum(probs[micro_index], axis=0)
        loss_terms.append(EXPERTS * (count_all / (MB_TOK * TOP)) * (prob_all / MB_TOK))
    return jnp.stack(outputs), jnp.stack(loss_terms)
```

```python
import jax
import jax.numpy as jnp
from jax import lax
from jax.experimental import pallas as pl
from jax.experimental.pallas import tpu as pltpu
from jax.sharding import PartitionSpec as P

MICRO = 2
CAP = 20
EXPERTS = 8
D = 4096
QUART = 1024
FFD = 896
ROWS = 80
HALF = 160
FULL = 320
SHIFTS = (0, 1, 3, 2)
NT = FFD // 128
MESH = pl.DeviceIdType.MESH
F32 = jnp.float32
BF16 = jnp.bfloat16


class Sems:
    def __init__(self):
        self.names = {}

    def __call__(self, *name):
        return self.names.setdefault(name, len(self.names))


N_SEND = 160
N_RECV = 160


def moe_kernel(
    tok_ref, meta_ref, wg_ref, wu_ref, wd_ref, out_ref, aux_ref,
    wgu, wdn, X, H, S, tok2, meta2, acc, R, DS, DR, OWN, T1, T2, T3, RR1, RR2, fin_in,
    stat_out, stat_in, stat_pair,
    wsem, ssem, rsem,
):
    dp = lax.axis_index("dp")
    y = lax.axis_index("tensor")
    x = dp // 8
    z = (dp // 2) % 4
    c = dp % 2
    zb = z % 2
    zh = z // 2

    def at(xx, zz, cc):
        return (xx * 8 + zz * 2 + cc, y)

    up = (dp, (y + 1) % 4)
    dn = (dp, (y + 3) % 4)
    partner = at(x, z, 1 - c)
    dests = [[at((x + 4 - s) % 4, 2 * c + i, 1 - zh) for i in range(2)] for s in SHIFTS]
    sources = [[at((x + s) % 4, 2 * (1 - c) + b, zh) for b in range(2)] for s in SHIFTS]

    send_ids, recv_ids = Sems(), Sems()
    pending = {}

    def msg(src, dst, dev, recv, offset=0):
        return pltpu.make_async_remote_copy(
            src_ref=src, dst_ref=dst, send_sem=None, recv_sem=rsem.at[recv + offset],
            device_id=dev, device_id_type=MESH,
        )

    def send(name, src, dst, dev, recv):
        copy = pltpu.make_async_remote_copy(
            src_ref=src, dst_ref=dst, send_sem=ssem.at[send_ids(*name)], recv_sem=rsem.at[recv],
            device_id=dev, device_id_type=MESH,
        )
        copy.start()
        pending[name] = copy

    def sent(*name):
        if name in pending:
            pending.pop(name).wait_send()

    def arrived(dst, recv):
        pltpu.make_async_remote_copy(
            src_ref=dst, dst_ref=dst, send_sem=ssem.at[0], recv_sem=rsem.at[recv],
            device_id=partner, device_id_type=MESH,
        ).wait_recv()

    P1 = [[recv_ids("p1", k, b) for b in range(2)] for k in range(4)]
    ST = [recv_ids("st", i) for i in range(8)]
    P3 = [[recv_ids("p3", k, i) for i in range(2)] for k in range(4)]

    barrier = pltpu.get_barrier_semaphore()
    greeted = [up, dn, partner]
    for k in range(4):
        greeted += dests[k] + sources[k]
    for dev in greeted:
        pl.semaphore_signal(barrier, inc=1, device_id=dev, device_id_type=MESH)

    wcopies = []
    for n in range(NT):
        cols = pl.ds(n * 128, 128)
        wcopies.append([
            pltpu.make_async_copy(wg_ref.at[:, cols], wgu.at[n, :, pl.ds(0, 128)], wsem.at[2 * n]),
            pltpu.make_async_copy(wu_ref.at[:, cols], wgu.at[n, :, pl.ds(128, 128)], wsem.at[2 * n + 1]),
        ])
    dcopy = pltpu.make_async_copy(wd_ref, wdn, wsem.at[2 * NT])
    for pair in wcopies:
        for copy in pair:
            copy.start()
    dcopy.start()

    meta2[0:128, :] = meta_ref[...]
    tok2[0:128, :] = tok_ref[...]
    pl.semaphore_wait(barrier, len(greeted))

    send(("meta",), meta_ref, meta2.at[pl.ds(128, 128)], partner, recv_ids("meta"))
    send(("tok",), tok_ref, tok2.at[pl.ds(128, 128)], partner, recv_ids("tok"))

    rid = lax.broadcasted_iota(jnp.int32, (256, 256), 0)
    cid = lax.broadcasted_iota(jnp.int32, (256, 256), 1)
    lower = jnp.where((rid // 64 == cid // 64) & (rid > cid), 1.0, 0.0).astype(BF16)
    arrived(meta2.at[pl.ds(128, 128)], recv_ids("meta"))
    meta = meta2[...]
    lane = lax.broadcasted_iota(jnp.int32, (256, 128), 1).astype(F32)
    r0, r1 = meta[:, 8:9], meta[:, 9:10]
    oh0 = jnp.where(lane == r0, 1.0, 0.0)
    oh1 = jnp.where(lane == r1, 1.0, 0.0)
    both = oh0 + oh1
    before = jnp.dot(lower, both.astype(BF16), preferred_element_type=F32)
    place0 = jnp.sum(before * oh0, axis=1, keepdims=True)
    place1 = jnp.sum(before * oh1, axis=1, keepdims=True)
    p0 = jnp.sum(meta * oh0, axis=1, keepdims=True)
    p1 = jnp.sum(meta * oh1, axis=1, keepdims=True)
    w0 = p0 / (p0 + p1)
    w1 = p1 / (p0 + p1)
    base = ((lax.broadcasted_iota(jnp.int32, (256, 1), 0) // 64) * CAP).astype(F32)
    s0 = base + place0
    s1 = base + place1

    def columns(k):
        e = (2 * ((x + 4 - SHIFTS[k]) % 4) + c).astype(F32)
        return jnp.where(r0 == e, s0, -1.0), jnp.where(r1 == e, s1, -1.0)

    def two_rows(v):
        a = jnp.sum(v[0:64] , axis=0, keepdims=True) + jnp.sum(v[128:192], axis=0, keepdims=True)
        b = jnp.sum(v[64:128], axis=0, keepdims=True) + jnp.sum(v[192:256], axis=0, keepdims=True)
        return a, b

    ca, cb = two_rows(both)
    pa, pb = two_rows(meta)
    stat_out[...] = jnp.concatenate([ca, cb, pa, pb, jnp.zeros((4, 128), F32)], axis=0)

    arrived(tok2.at[pl.ds(128, 128)], recv_ids("tok"))
    slot_lane = lax.broadcasted_iota(jnp.int32, (256, ROWS), 1).astype(F32)
    for k in range(4):
        c0, c1 = columns(k)
        place = (jnp.where(slot_lane == c0, 1.0, 0.0) + jnp.where(slot_lane == c1, 1.0, 0.0)).astype(BF16)
        S[k] = lax.dot_general(
            place, tok2[...], (((0,), (0,)), ((), ())), preferred_element_type=F32
        ).astype(BF16)
        for i in range(2):
            send(("p1", k, i), S.at[k], X.at[k, 0, pl.ds(pl.multiple_of(zb * ROWS, 16), ROWS)],
                 dests[k][i], P1[k][0] + zb)
            send(("st", k, i), stat_out, stat_in.at[x * 2 + zb], dests[k][i], ST[0] + x * 2 + zb)

    own = lambda b: pl.ds(b * ROWS, ROWS)
    other = lambda b: pl.ds(HALF + b * ROWS, ROWS)

    def to_partner(k, r, b):
        send(("d", k, r, b), X.at[k, r, own(b)], X.at[k, r, other(b)], partner, recv_ids("d", k, r, b))

    def gather_start(k):
        for b in range(2):
            arrived(X.at[k, 0, own(b)], P1[k][b])
            send(("u", k, b), X.at[k, 0, own(b)], X.at[k, 3, own(b)], up, recv_ids("u", k, b))
            send(("n", k, b), X.at[k, 0, own(b)], X.at[k, 1, own(b)], dn, recv_ids("n", k, b))
            to_partner(k, 0, b)

    def gather_forward(k):
        arrived(X.at[k, 3, own(0)], recv_ids("u", k, 0))
        send(("fu", k), X.at[k, 3, own(0)], X.at[k, 2, own(0)], up, recv_ids("fu", k))
        to_partner(k, 3, 0)
        arrived(X.at[k, 1, own(0)], recv_ids("n", k, 0))
        to_partner(k, 1, 0)
        arrived(X.at[k, 1, own(1)], recv_ids("n", k, 1))
        send(("fn", k), X.at[k, 1, own(1)], X.at[k, 2, own(1)], dn, recv_ids("fn", k))
        to_partner(k, 1, 1)
        arrived(X.at[k, 3, own(1)], recv_ids("u", k, 1))
        to_partner(k, 3, 1)

    def gather_end(k):
        arrived(X.at[k, 2, own(0)], recv_ids("fu", k))
        to_partner(k, 2, 0)
        arrived(X.at[k, 2, own(1)], recv_ids("fn", k))
        to_partner(k, 2, 1)

    def gathered(k):
        for r in (0, 3, 1, 2):
            for b in range(2):
                arrived(X.at[k, r, other(b)], recv_ids("d", k, r, b))

    def hidden(k, start, stop):
        def step(n, carry):
            total = None
            for r in range(4):
                rows = pl.ds(pl.multiple_of(((y + r) % 4) * QUART, QUART), QUART)
                term = jnp.dot(X[k, r], wgu[n, rows, :], preferred_element_type=F32)
                total = term if total is None else total + term
            gate, up_ = total[:, :128], total[:, 128:]
            value = gate / (1.0 + jnp.exp(-gate)) * up_
            H[:, pl.ds(pl.multiple_of(n * 128, 128), 128)] = value.astype(BF16)
            return carry

        if k == 0:
            for n in range(start, stop):
                for copy in wcopies[n]:
                    copy.wait()
        lax.fori_loop(start, stop, step, 0)

    def down(k):
        slot = k % 2
        if k == 0:
            dcopy.wait()
        for r in range(4):
            sent("ds", k - 2, r)

        def step(i, carry):
            r = 2 - i
            r = jnp.where(r < 0, 3, r)
            cols = pl.ds(pl.multiple_of(((y + r) % 4) * QUART, QUART), QUART)
            part = jnp.dot(H[...], wdn[:, cols], preferred_element_type=F32)
            OWN[slot, r] = part[:HALF]
            DS[slot, r] = part[HALF:].astype(BF16)
            return carry

        lax.fori_loop(0, 4, step, 0)
        for r in (2, 1, 3, 0):
            send(("ds", k, r), DS.at[slot, r], DR.at[k, r], partner, recv_ids("ds", k, r))

    def chip_sum(k, r):
        arrived(DR.at[k, r], recv_ids("ds", k, r))
        return OWN[k % 2, r] + DR[k, r].astype(F32)

    def scatter_start(k):
        slot = k % 2
        sent("a1", k - 2)
        sent("b1", k - 2)
        T1[slot] = chip_sum(k, 2).astype(BF16)
        send(("a1", k), T1.at[slot, pl.ds(0, ROWS)], RR1.at[k, 0], dn, recv_ids("a1", k))
        send(("b1", k), T1.at[slot, pl.ds(ROWS, ROWS)], RR1.at[k, 1], up, recv_ids("b1", k))

    def scatter_forward(k):
        slot = k % 2
        sent("a2", k - 2)
        sent("b2", k - 2)
        total = chip_sum(k, 3)
        arrived(RR1.at[k, 0], recv_ids("a1", k))
        T2[slot, 0, 0:ROWS] = (total[:ROWS] + RR1[k, 0].astype(F32)).astype(BF16)
        T2[slot, 0, ROWS:HALF] = total[ROWS:].astype(BF16)
        send(("a2", k), T2.at[slot, 0], RR2.at[k, 0], dn, recv_ids("a2", k))
        total = chip_sum(k, 1)
        arrived(RR1.at[k, 1], recv_ids("b1", k))
        T2[slot, 1, 0:ROWS] = total[:ROWS].astype(BF16)
        T2[slot, 1, ROWS:HALF] = (total[ROWS:] + RR1[k, 1].astype(F32)).astype(BF16)
        send(("b2", k), T2.at[slot, 1], RR2.at[k, 1], up, recv_ids("b2", k))

    def scatter_end(k):
        slot = k % 2
        for b in range(2):
            sent("p3", k - 2, b)
        total = chip_sum(k, 0)
        arrived(RR2.at[k, 0], recv_ids("a2", k))
        arrived(RR2.at[k, 1], recv_ids("b2", k))
        T3[slot] = (total + RR2[k, 0].astype(F32) + RR2[k, 1].astype(F32)).astype(BF16)
        for b in range(2):
            send(("p3", k, b), T3.at[slot, own(b)], R.at[k, pl.ds(pl.multiple_of(zb * ROWS, 16), ROWS)],
                 sources[k][b], P3[k][0] + zb)

    two_lane = lax.broadcasted_iota(jnp.int32, (256, HALF), 1)
    two_lane = jnp.where(two_lane >= ROWS, two_lane - ROWS, two_lane).astype(F32)

    def combine(k):
        for i in range(2):
            arrived(R.at[k, own(i)], P3[k][i])
        c0, c1 = columns(k)
        weight = jnp.where(two_lane == c0, w0, 0.0) + jnp.where(two_lane == c1, w1, 0.0)
        high = weight.astype(BF16)
        low = (weight - high.astype(F32)).astype(BF16)
        rows = R[k]
        term = jnp.dot(high, rows, preferred_element_type=F32) + jnp.dot(
            low, rows, preferred_element_type=F32
        )
        acc[...] = term if k == 0 else acc[...] + term

    gather_start(0)
    gather_start(1)
    gather_forward(0)
    gather_start(2)
    gather_end(0)
    for i in range(8):
        arrived(stat_in.at[i], ST[i])
    total = stat_in[0]
    for i in range(1, 8):
        total = total + stat_in[i]
    stat_pair[0] = total
    send(("sp",), stat_pair.at[0], stat_pair.at[1], partner, recv_ids("sp"))
    gathered(0)

    hidden(0, 0, 4)
    gather_forward(1)
    gather_start(3)
    hidden(0, 4, NT)
    gather_end(1)
    down(0)
    gathered(1)

    hidden(1, 0, 4)
    scatter_start(0)
    gather_forward(2)
    hidden(1, 4, NT)
    gather_end(2)
    scatter_forward(0)
    down(1)
    gathered(2)

    hidden(2, 0, 4)
    scatter_end(0)
    scatter_start(1)
    gather_forward(3)
    hidden(2, 4, NT)
    scatter_forward(1)
    gather_end(3)
    down(2)
    gathered(3)

    hidden(3, 0, 4)
    scatter_end(1)
    scatter_start(2)
    hidden(3, 4, NT)
    scatter_forward(2)
    combine(0)
    down(3)

    scatter_start(3)
    scatter_end(2)
    combine(1)
    scatter_forward(3)
    arrived(stat_pair.at[1], recv_ids("sp"))
    total = stat_pair[0] + stat_pair[1]
    aux_ref[...] = EXPERTS * (total[0:2, 0:8] / 4096.0) * (total[2:4, 0:8] / 2048.0)
    combine(2)
    scatter_end(3)
    combine(3)
    send(("fin",), acc.at[pl.ds(128, 128)], fin_in, partner, recv_ids("fin"))
    arrived(fin_in, recv_ids("fin"))
    out_ref[...] = (acc[0:128, :] + fin_in[...]).astype(BF16)
    for name in list(pending):
        sent(*name)
    assert len(send_ids.names) <= N_SEND and len(recv_ids.names) <= N_RECV


def local(tokens, routes, probs, w_gate, w_up, w_down):
    meta = jnp.concatenate(
        [probs.reshape(128, EXPERTS), routes.reshape(128, 2).astype(F32), jnp.zeros((128, 118), F32)], axis=1
    )
    vmem = pl.BlockSpec(memory_space=pltpu.VMEM)
    hbm = pl.BlockSpec(memory_space=pl.ANY)
    mixed, aux = pl.pallas_call(
        moe_kernel,
        out_shape=(jax.ShapeDtypeStruct((128, QUART), BF16), jax.ShapeDtypeStruct((2, 8), F32)),
        in_specs=[vmem, vmem, hbm, hbm, hbm],
        out_specs=(vmem, vmem),
        scratch_shapes=[
            pltpu.VMEM((NT, D, 256), BF16),
            pltpu.VMEM((FFD, D), BF16),
            pltpu.VMEM((4, 4, FULL, QUART), BF16),
            pltpu.VMEM((FULL, FFD), BF16),
            pltpu.VMEM((4, ROWS, QUART), BF16),
            pltpu.VMEM((256, QUART), BF16),
            pltpu.VMEM((256, 128), F32),
            pltpu.VMEM((256, QUART), F32),
            pltpu.VMEM((4, HALF, QUART), BF16),
            pltpu.VMEM((2, 4, HALF, QUART), BF16),
            pltpu.VMEM((4, 4, HALF, QUART), BF16),
            pltpu.VMEM((2, 4, HALF, QUART), F32),
            pltpu.VMEM((2, HALF, QUART), BF16),
            pltpu.VMEM((2, 2, HALF, QUART), BF16),
            pltpu.VMEM((2, HALF, QUART), BF16),
            pltpu.VMEM((4, 2, ROWS, QUART), BF16),
            pltpu.VMEM((4, 2, HALF, QUART), BF16),
            pltpu.VMEM((128, QUART), F32),
            pltpu.VMEM((8, 128), F32),
            pltpu.VMEM((8, 8, 128), F32),
            pltpu.VMEM((2, 8, 128), F32),
            pltpu.SemaphoreType.DMA((2 * NT + 1,)),
            pltpu.SemaphoreType.DMA((N_SEND,)),
            pltpu.SemaphoreType.DMA((N_RECV,)),
        ],
        compiler_params=pltpu.CompilerParams(
            collective_id=0, has_side_effects=True, vmem_limit_bytes=66_000_000
        ),
        name="moe",
    )(tokens.reshape(128, QUART), meta, w_gate[0], w_up[0], w_down[0])
    return mixed.reshape(MICRO, 64, QUART), aux


def solution(mesh):
    in_specs = (
        P(None, "dp", "tensor"),
        P(None, "dp", None),
        P(None, "dp", None),
        P("dp", None, "tensor"),
        P("dp", None, "tensor"),
        P("dp", "tensor", None),
    )
    out_specs = (P(None, "dp", "tensor"), P())
    return jax.shard_map(local, mesh=mesh, in_specs=in_specs, out_specs=out_specs, check_vma=False)
```

```python
import jax
import jax.numpy as jnp
from jax import lax
from jax.experimental import pallas as pl
from jax.experimental.pallas import tpu as pltpu
from jax.sharding import PartitionSpec as P

MICRO = 2
CAP = 20
EXPERTS = 8
D = 4096
QUART = 1024
FFD = 896
ROWS = 80
HALF = 160
FULL = 320
WT = 256
WS = QUART - WT
SHIFTS = (1, 3, 2, 0)
NT = FFD // 128
MESH = pl.DeviceIdType.MESH
F32 = jnp.float32
BF16 = jnp.bfloat16


class Sems:
    def __init__(self):
        self.names = {}

    def __call__(self, *name):
        return self.names.setdefault(name, len(self.names))


N_SEND = 200
N_RECV = 200


def moe_kernel(
    tok_ref, meta_ref, wg_ref, wu_ref, wd_ref, out_ref, aux_ref,
    wgu, wdn, X, H, S, TS, tok2, tokT, PL, meta2, acc, accT, R, RT, DS, DR, OWN, T1, T2, T3, T4, RR1, RR2,
    fin_in, finT_in, YS, YR,
    stat_out, stat_in, stat_pair,
    wsem, ssem, rsem,
):
    dp = lax.axis_index("dp")
    y = lax.axis_index("tensor")
    x = dp // 8
    z = (dp // 2) % 4
    c = dp % 2
    zb = z % 2
    zh = z // 2

    def at(xx, zz, cc):
        return (xx * 8 + zz * 2 + cc, y)

    up = (dp, (y + 1) % 4)
    dn = (dp, (y + 3) % 4)
    far = (dp, (y + 2) % 4)
    round_y = {1: up, 2: far, 3: dn}
    partner = at(x, z, 1 - c)
    dests = [[at((x + 4 - s) % 4, 2 * c + i, 1 - zh) for i in range(2)] for s in SHIFTS]
    sources = [[at((x + s) % 4, 2 * (1 - c) + b, zh) for b in range(2)] for s in SHIFTS]

    send_ids, recv_ids = Sems(), Sems()
    pending = {}

    def msg(src, dst, dev, recv, offset=0):
        return pltpu.make_async_remote_copy(
            src_ref=src, dst_ref=dst, send_sem=None, recv_sem=rsem.at[recv + offset],
            device_id=dev, device_id_type=MESH,
        )

    def send(name, src, dst, dev, recv):
        copy = pltpu.make_async_remote_copy(
            src_ref=src, dst_ref=dst, send_sem=ssem.at[send_ids(*name)], recv_sem=rsem.at[recv],
            device_id=dev, device_id_type=MESH,
        )
        copy.start()
        pending[name] = copy

    def sent(*name):
        if name in pending:
            pending.pop(name).wait_send()

    def arrived(dst, recv):
        pltpu.make_async_remote_copy(
            src_ref=dst, dst_ref=dst, send_sem=ssem.at[0], recv_sem=rsem.at[recv],
            device_id=partner, device_id_type=MESH,
        ).wait_recv()

    P1 = [[recv_ids("p1", k, b) for b in range(2)] for k in range(4)]
    ST = [recv_ids("st", i) for i in range(8)]
    P3 = [[recv_ids("p3", k, i) for i in range(2)] for k in range(4)]
    P1T = [[recv_ids("p1t", k, b) for b in range(2)] for k in range(4)]
    P3T = [[recv_ids("p3t", k, i) for i in range(2)] for k in range(4)]

    barrier = pltpu.get_barrier_semaphore()
    greeted = [up, dn, far, partner]
    for k in range(4):
        greeted += dests[k] + sources[k]
    for dev in greeted:
        pl.semaphore_signal(barrier, inc=1, device_id=dev, device_id_type=MESH)

    wcopies = []
    for n in range(NT):
        cols = pl.ds(n * 128, 128)
        wcopies.append([
            pltpu.make_async_copy(wg_ref.at[:, cols], wgu.at[n, :, pl.ds(0, 128)], wsem.at[2 * n]),
            pltpu.make_async_copy(wu_ref.at[:, cols], wgu.at[n, :, pl.ds(128, 128)], wsem.at[2 * n + 1]),
        ])
    dcopy = pltpu.make_async_copy(wd_ref, wdn, wsem.at[2 * NT])
    for pair in wcopies:
        for copy in pair:
            copy.start()
    dcopy.start()

    meta2[0:128, :] = meta_ref[...]
    tok2[0:128, :] = tok_ref[...]
    pl.semaphore_wait(barrier, len(greeted))

    send(("meta",), meta_ref, meta2.at[pl.ds(128, 128)], partner, recv_ids("meta"))
    send(("tok",), tok_ref, tok2.at[pl.ds(128, 128)], partner, recv_ids("tok"))
    tcols = pl.ds(WS, WT)
    scols = pl.ds(0, WS)
    mine, theirs = pl.ds(0, 128), pl.ds(128, 128)
    for r in (1, 3, 2):
        send(("ty", r), tok_ref.at[:, tcols], tokT.at[4 - r, mine], round_y[r], recv_ids("ty", 4 - r))

    rid = lax.broadcasted_iota(jnp.int32, (256, 256), 0)
    cid = lax.broadcasted_iota(jnp.int32, (256, 256), 1)
    lower = jnp.where((rid // 64 == cid // 64) & (rid > cid), 1.0, 0.0).astype(BF16)
    arrived(meta2.at[pl.ds(128, 128)], recv_ids("meta"))
    meta = meta2[...]
    lane = lax.broadcasted_iota(jnp.int32, (256, 128), 1).astype(F32)
    r0, r1 = meta[:, 8:9], meta[:, 9:10]
    oh0 = jnp.where(lane == r0, 1.0, 0.0)
    oh1 = jnp.where(lane == r1, 1.0, 0.0)
    both = oh0 + oh1
    before = jnp.dot(lower, both.astype(BF16), preferred_element_type=F32)
    place0 = jnp.sum(before * oh0, axis=1, keepdims=True)
    place1 = jnp.sum(before * oh1, axis=1, keepdims=True)
    p0 = jnp.sum(meta * oh0, axis=1, keepdims=True)
    p1 = jnp.sum(meta * oh1, axis=1, keepdims=True)
    w0 = p0 / (p0 + p1)
    w1 = p1 / (p0 + p1)
    base = ((lax.broadcasted_iota(jnp.int32, (256, 1), 0) // 64) * CAP).astype(F32)
    s0 = base + place0
    s1 = base + place1

    def columns(k):
        e = (2 * ((x + 4 - SHIFTS[k]) % 4) + c).astype(F32)
        return jnp.where(r0 == e, s0, -1.0), jnp.where(r1 == e, s1, -1.0)

    def two_rows(v):
        a = jnp.sum(v[0:64] , axis=0, keepdims=True) + jnp.sum(v[128:192], axis=0, keepdims=True)
        b = jnp.sum(v[64:128], axis=0, keepdims=True) + jnp.sum(v[192:256], axis=0, keepdims=True)
        return a, b

    ca, cb = two_rows(both)
    pa, pb = two_rows(meta)
    stat_out[...] = jnp.concatenate([ca, cb, pa, pb, jnp.zeros((4, 128), F32)], axis=0)

    arrived(tok2.at[pl.ds(128, 128)], recv_ids("tok"))
    slot_lane = lax.broadcasted_iota(jnp.int32, (256, ROWS), 1).astype(F32)
    block = pl.ds(pl.multiple_of(zb * ROWS, 16), ROWS)

    def slots(k, rows):
        return lax.dot_general(
            PL[k], rows, (((0,), (0,)), ((), ())), preferred_element_type=F32
        ).astype(BF16)

    def dispatch(k):
        c0, c1 = columns(k)
        PL[k] = (jnp.where(slot_lane == c0, 1.0, 0.0) + jnp.where(slot_lane == c1, 1.0, 0.0)).astype(BF16)
        S[k] = slots(k, tok2[:, 0:WS])
        for i in range(2):
            send(("p1", k, i), S.at[k], X.at[k, 0, block, scols], dests[k][i], P1[k][0] + zb)

    def tokens_along_y():
        for r in (1, 3, 2):
            arrived(tokT.at[r, mine], recv_ids("ty", r))
            send(("td", r), tokT.at[r, mine], tokT.at[r, theirs], partner, recv_ids("td", r))
        for r in (1, 3, 2):
            arrived(tokT.at[r, theirs], recv_ids("td", r))

    def dispatch_direct(k):
        TS[k, 0] = slots(k, tok2[:, WS:QUART])
        for r in range(1, 4):
            TS[k, r] = slots(k, tokT[r])
        for i in range(2):
            send(("p1t", k, i), TS.at[k], X.at[k, :, block, tcols], dests[k][i], P1T[k][0] + zb)

    def dispatch_stats():
        for k in range(4):
            for i in range(2):
                send(("st", k, i), stat_out, stat_in.at[x * 2 + zb], dests[k][i], ST[0] + x * 2 + zb)

    own = lambda b: pl.ds(b * ROWS, ROWS)
    other = lambda b: pl.ds(HALF + b * ROWS, ROWS)

    def to_partner(k, r, b):
        send(("d", k, r, b), X.at[k, r, own(b), scols], X.at[k, r, other(b), scols], partner,
             recv_ids("d", k, r, b))

    def gather_start(k):
        for b in range(2):
            arrived(X.at[k, 0, own(b), scols], P1[k][b])
            send(("u", k, b), X.at[k, 0, own(b), scols], X.at[k, 3, own(b), scols], up, recv_ids("u", k, b))
            send(("n", k, b), X.at[k, 0, own(b), scols], X.at[k, 1, own(b), scols], dn, recv_ids("n", k, b))
            to_partner(k, 0, b)

    def gather_forward(k):
        arrived(X.at[k, 3, own(0), scols], recv_ids("u", k, 0))
        send(("fu", k), X.at[k, 3, own(0), scols], X.at[k, 2, own(0), scols], up, recv_ids("fu", k))
        to_partner(k, 3, 0)
        arrived(X.at[k, 1, own(0), scols], recv_ids("n", k, 0))
        to_partner(k, 1, 0)
        arrived(X.at[k, 1, own(1), scols], recv_ids("n", k, 1))
        send(("fn", k), X.at[k, 1, own(1), scols], X.at[k, 2, own(1), scols], dn, recv_ids("fn", k))
        to_partner(k, 1, 1)
        arrived(X.at[k, 3, own(1), scols], recv_ids("u", k, 1))
        to_partner(k, 3, 1)

    def gather_direct(k):
        for b in range(2):
            arrived(X.at[k, :, own(b), tcols], P1T[k][b])
            send(("dt", k, b), X.at[k, :, own(b), tcols], X.at[k, :, other(b), tcols], partner,
                 recv_ids("dt", k, b))

    def gather_end(k):
        arrived(X.at[k, 2, own(0), scols], recv_ids("fu", k))
        to_partner(k, 2, 0)
        arrived(X.at[k, 2, own(1), scols], recv_ids("fn", k))
        to_partner(k, 2, 1)
        gather_direct(k)

    def gathered(k):
        for r in (0, 3, 1, 2):
            for b in range(2):
                arrived(X.at[k, r, other(b), scols], recv_ids("d", k, r, b))
        for b in range(2):
            arrived(X.at[k, :, other(b), tcols], recv_ids("dt", k, b))

    def hidden(k, start, stop):
        def tile(n):
            total = None
            for r in range(4):
                rows = pl.ds(pl.multiple_of(((y + r) % 4) * QUART, QUART), QUART)
                term = jnp.dot(X[k, r], wgu[n, rows, :], preferred_element_type=F32)
                total = term if total is None else total + term
            gate, up_ = total[:, :128], total[:, 128:]
            value = gate / (1.0 + jnp.exp(-gate)) * up_
            first = n * 128 if isinstance(n, int) else pl.multiple_of(n * 128, 128)
            H[:, pl.ds(first, 128)] = value.astype(BF16)

        def step(i, carry):
            tile(start + 2 * i)
            tile(start + 2 * i + 1)
            return carry

        if k == 0:
            for n in range(start, stop):
                for copy in wcopies[n]:
                    copy.wait()
        lax.fori_loop(0, (stop - start) // 2, step, 0)
        if (stop - start) % 2:
            tile(stop - 1)

    def down(k):
        slot = k % 2
        if k == 0:
            dcopy.wait()
        for r in range(4):
            sent("ds", k - 2, r)

        def quarter(r):
            cols = pl.ds(pl.multiple_of(((y + r) % 4) * QUART, QUART), QUART)
            part = jnp.dot(H[...], wdn[:, cols], preferred_element_type=F32)
            OWN[slot, r] = part[:HALF]
            DS[slot, r] = part[HALF:].astype(BF16)

        def share(r):
            send(("ds", k, r), DS.at[slot, r], DR.at[k, r], partner, recv_ids("ds", k, r))

        def step(i, carry):
            quarter(2 + i)
            quarter(1 - i)
            return carry

        if k < 3:
            lax.fori_loop(0, 2, step, 0)
            for r in (2, 1, 3, 0):
                share(r)
        else:
            for r in (2, 1, 3, 0):
                quarter(r)
                share(r)

    shared = set()

    def chip_sum(k, r, a, b):
        if (k, r) not in shared:
            shared.add((k, r))
            arrived(DR.at[k, r], recv_ids("ds", k, r))
        return OWN[k % 2, r, :, a:b] + DR[k, r, :, a:b].astype(F32)

    def scatter_start(k):
        slot = k % 2
        sent("a1", k - 2)
        sent("b1", k - 2)
        T1[slot] = chip_sum(k, 2, 0, WS).astype(BF16)
        send(("a1", k), T1.at[slot, pl.ds(0, ROWS)], RR1.at[k, 0], dn, recv_ids("a1", k))
        send(("b1", k), T1.at[slot, pl.ds(ROWS, ROWS)], RR1.at[k, 1], up, recv_ids("b1", k))
        for b in range(2):
            sent("p3t", k - 2, b)
        for r in (2, 1, 3, 0):
            T4[slot, r] = chip_sum(k, r, WS, QUART).astype(BF16)
        for b in range(2):
            send(("p3t", k, b), T4.at[slot, :, own(b)], RT.at[k, :, block], sources[k][b], P3T[k][0] + zb)

    def scatter_forward(k):
        slot = k % 2
        sent("a2", k - 2)
        sent("b2", k - 2)
        total = chip_sum(k, 3, 0, WS)
        arrived(RR1.at[k, 0], recv_ids("a1", k))
        T2[slot, 0, 0:ROWS] = (total[:ROWS] + RR1[k, 0].astype(F32)).astype(BF16)
        T2[slot, 0, ROWS:HALF] = total[ROWS:].astype(BF16)
        send(("a2", k), T2.at[slot, 0], RR2.at[k, 0], dn, recv_ids("a2", k))
        total = chip_sum(k, 1, 0, WS)
        arrived(RR1.at[k, 1], recv_ids("b1", k))
        T2[slot, 1, 0:ROWS] = total[:ROWS].astype(BF16)
        T2[slot, 1, ROWS:HALF] = (total[ROWS:] + RR1[k, 1].astype(F32)).astype(BF16)
        send(("b2", k), T2.at[slot, 1], RR2.at[k, 1], up, recv_ids("b2", k))

    def scatter_end(k):
        slot = k % 2
        for b in range(2):
            sent("p3", k - 2, b)
        total = chip_sum(k, 0, 0, WS)
        arrived(RR2.at[k, 0], recv_ids("a2", k))
        arrived(RR2.at[k, 1], recv_ids("b2", k))
        T3[slot] = (total + RR2[k, 0].astype(F32) + RR2[k, 1].astype(F32)).astype(BF16)
        for b in range(2):
            send(("p3", k, b), T3.at[slot, own(b)], R.at[k, block], sources[k][b], P3[k][0] + zb)

    two_lane = lax.broadcasted_iota(jnp.int32, (256, HALF), 1)
    two_lane = jnp.where(two_lane >= ROWS, two_lane - ROWS, two_lane).astype(F32)

    def weights(k):
        c0, c1 = columns(k)
        weight = jnp.where(two_lane == c0, w0, 0.0) + jnp.where(two_lane == c1, w1, 0.0)
        high = weight.astype(BF16)
        return high, (weight - high.astype(F32)).astype(BF16)

    def mix(high, low, rows):
        return jnp.dot(high, rows, preferred_element_type=F32) + jnp.dot(
            low, rows, preferred_element_type=F32
        )

    def combine_direct(k):
        for i in range(2):
            arrived(RT.at[k, :, own(i)], P3T[k][i])
        high, low = weights(k)
        for r in range(4):
            term = mix(high, low, RT[k, r])
            accT[r] = term if k == 0 else accT[r] + term

    def combine(k):
        for i in range(2):
            arrived(R.at[k, own(i)], P3[k][i])
        high, low = weights(k)
        term = mix(high, low, R[k])
        acc[...] = term if k == 0 else acc[...] + term

    dispatch(0)
    dispatch(1)
    tokens_along_y()
    dispatch_direct(0)
    gather_start(0)
    dispatch(2)
    dispatch(3)
    dispatch_direct(1)
    gather_start(1)
    gather_forward(0)
    dispatch_stats()
    gather_end(0)
    gathered(0)

    hidden(0, 0, 3)
    dispatch_direct(2)
    gather_forward(1)
    gather_start(2)
    hidden(0, 3, NT)
    dispatch_direct(3)
    gather_end(1)
    gather_start(3)
    for i in range(8):
        arrived(stat_in.at[i], ST[i])
    total = stat_in[0]
    for i in range(1, 8):
        total = total + stat_in[i]
    stat_pair[0] = total
    send(("sp",), stat_pair.at[0], stat_pair.at[1], partner, recv_ids("sp"))
    down(0)
    gather_forward(2)
    gathered(1)

    hidden(1, 0, 4)
    scatter_start(0)
    gather_end(2)
    hidden(1, 4, NT)
    gather_forward(3)
    scatter_forward(0)
    down(1)
    gathered(2)

    hidden(2, 0, 4)
    scatter_end(0)
    scatter_start(1)
    gather_end(3)
    hidden(2, 4, NT)
    scatter_forward(1)
    down(2)
    gathered(3)

    hidden(3, 0, 4)
    scatter_end(1)
    scatter_start(2)
    combine_direct(0)
    hidden(3, 4, NT)
    scatter_forward(2)
    combine(0)
    combine_direct(1)
    down(3)

    scatter_start(3)
    scatter_end(2)
    combine_direct(2)
    combine(1)
    scatter_forward(3)
    combine_direct(3)
    send(("finT",), accT.at[:, theirs], finT_in, partner, recv_ids("finT"))
    arrived(stat_pair.at[1], recv_ids("sp"))
    total = stat_pair[0] + stat_pair[1]
    aux_ref[...] = EXPERTS * (total[0:2, 0:8] / 4096.0) * (total[2:4, 0:8] / 2048.0)
    combine(2)
    arrived(finT_in, recv_ids("finT"))
    for r in (2, 1, 3):
        YS[r] = (accT[r, 0:128] + finT_in[r]).astype(BF16)
        send(("ys", r), YS.at[r], YR.at[r], round_y[r], recv_ids("ys", r))
    scatter_end(3)
    combine(3)
    send(("fin",), acc.at[theirs], fin_in, partner, recv_ids("fin"))
    total = accT[0, 0:128] + finT_in[0]
    for r in (1, 3, 2):
        arrived(YR.at[r], recv_ids("ys", r))
        total = total + YR[r].astype(F32)
    out_ref[:, WS:QUART] = total.astype(BF16)
    arrived(fin_in, recv_ids("fin"))
    out_ref[:, 0:WS] = (acc[0:128, :] + fin_in[...]).astype(BF16)
    for name in list(pending):
        sent(*name)
    assert len(send_ids.names) <= N_SEND and len(recv_ids.names) <= N_RECV


def local(tokens, routes, probs, w_gate, w_up, w_down):
    meta = jnp.concatenate(
        [probs.reshape(128, EXPERTS), routes.reshape(128, 2).astype(F32), jnp.zeros((128, 118), F32)], axis=1
    )
    vmem = pl.BlockSpec(memory_space=pltpu.VMEM)
    hbm = pl.BlockSpec(memory_space=pl.ANY)
    mixed, aux = pl.pallas_call(
        moe_kernel,
        out_shape=(jax.ShapeDtypeStruct((128, QUART), BF16), jax.ShapeDtypeStruct((2, 8), F32)),
        in_specs=[vmem, vmem, hbm, hbm, hbm],
        out_specs=(vmem, vmem),
        scratch_shapes=[
            pltpu.VMEM((NT, D, 256), BF16),
            pltpu.VMEM((FFD, D), BF16),
            pltpu.VMEM((4, 4, FULL, QUART), BF16),
            pltpu.VMEM((FULL, FFD), BF16),
            pltpu.VMEM((4, ROWS, WS), BF16),
            pltpu.VMEM((4, 4, ROWS, WT), BF16),
            pltpu.VMEM((256, QUART), BF16),
            pltpu.VMEM((4, 256, WT), BF16),
            pltpu.VMEM((4, 256, ROWS), BF16),
            pltpu.VMEM((256, 128), F32),
            pltpu.VMEM((256, WS), F32),
            pltpu.VMEM((4, 256, WT), F32),
            pltpu.VMEM((4, HALF, WS), BF16),
            pltpu.VMEM((4, 4, HALF, WT), BF16),
            pltpu.VMEM((2, 4, HALF, QUART), BF16),
            pltpu.VMEM((4, 4, HALF, QUART), BF16),
            pltpu.VMEM((2, 4, HALF, QUART), F32),
            pltpu.VMEM((2, HALF, WS), BF16),
            pltpu.VMEM((2, 2, HALF, WS), BF16),
            pltpu.VMEM((2, HALF, WS), BF16),
            pltpu.VMEM((2, 4, HALF, WT), BF16),
            pltpu.VMEM((4, 2, ROWS, WS), BF16),
            pltpu.VMEM((4, 2, HALF, WS), BF16),
            pltpu.VMEM((128, WS), F32),
            pltpu.VMEM((4, 128, WT), F32),
            pltpu.VMEM((4, 128, WT), BF16),
            pltpu.VMEM((4, 128, WT), BF16),
            pltpu.VMEM((8, 128), F32),
            pltpu.VMEM((8, 8, 128), F32),
            pltpu.VMEM((2, 8, 128), F32),
            pltpu.SemaphoreType.DMA((2 * NT + 1,)),
            pltpu.SemaphoreType.DMA((N_SEND,)),
            pltpu.SemaphoreType.DMA((N_RECV,)),
        ],
        compiler_params=pltpu.CompilerParams(
            collective_id=0, has_side_effects=True, vmem_limit_bytes=66_000_000
        ),
        name="moe",
    )(tokens.reshape(128, QUART), meta, w_gate[0], w_up[0], w_down[0])
    return mixed.reshape(MICRO, 64, QUART), aux


def solution(mesh):
    in_specs = (
        P(None, "dp", "tensor"),
        P(None, "dp", None),
        P(None, "dp", None),
        P("dp", None, "tensor"),
        P("dp", None, "tensor"),
        P("dp", "tensor", None),
    )
    out_specs = (P(None, "dp", "tensor"), P())
    return jax.shard_map(local, mesh=mesh, in_specs=in_specs, out_specs=out_specs, check_vma=False)
```

```python
import jax
import jax.numpy as jnp
from jax import lax
from jax.experimental import pallas as pl
from jax.experimental.pallas import tpu as pltpu
from jax.sharding import PartitionSpec as P

MICRO = 2
CAP = 20
EXPERTS = 8
D = 4096
QUART = 1024
FFD = 896
ROWS = 80
HALF = 160
FULL = 320
WT = 256
WS = QUART - WT
SHIFTS = (1, 3, 2, 0)
NT = FFD // 128
MESH = pl.DeviceIdType.MESH
F32 = jnp.float32
BF16 = jnp.bfloat16


class Sems:
    def __init__(self):
        self.names = {}

    def __call__(self, *name):
        return self.names.setdefault(name, len(self.names))


N_SEND = 200
N_RECV = 200


def moe_kernel(
    tok_ref, meta_ref, wg_ref, wu_ref, wd_ref, out_ref, aux_ref,
    wgu, wdn, X, H, S, TS, tok2, tokT, PL, meta2, acc, accT, R, RT, DS, DR, OWN, T1, T2, T3, T4, RR1, RR2,
    fin_in, finT_in, YS, YR,
    stat_out, stat_in, stat_pair,
    wsem, ssem, rsem,
):
    dp = lax.axis_index("dp")
    y = lax.axis_index("tensor")
    x = dp // 8
    z = (dp // 2) % 4
    c = dp % 2
    zb = z % 2
    zh = z // 2

    def at(xx, zz, cc):
        return (xx * 8 + zz * 2 + cc, y)

    up = (dp, (y + 1) % 4)
    dn = (dp, (y + 3) % 4)
    far = (dp, (y + 2) % 4)
    round_y = {1: up, 2: far, 3: dn}
    partner = at(x, z, 1 - c)
    dests = [[at((x + 4 - s) % 4, 2 * c + i, 1 - zh) for i in range(2)] for s in SHIFTS]
    sources = [[at((x + s) % 4, 2 * (1 - c) + b, zh) for b in range(2)] for s in SHIFTS]

    send_ids, recv_ids = Sems(), Sems()
    pending = {}

    def msg(src, dst, dev, recv, offset=0):
        return pltpu.make_async_remote_copy(
            src_ref=src, dst_ref=dst, send_sem=None, recv_sem=rsem.at[recv + offset],
            device_id=dev, device_id_type=MESH,
        )

    def send(name, src, dst, dev, recv):
        copy = pltpu.make_async_remote_copy(
            src_ref=src, dst_ref=dst, send_sem=ssem.at[send_ids(*name)], recv_sem=rsem.at[recv],
            device_id=dev, device_id_type=MESH,
        )
        copy.start()
        pending[name] = copy

    def sent(*name):
        if name in pending:
            pending.pop(name).wait_send()

    def arrived(dst, recv):
        pltpu.make_async_remote_copy(
            src_ref=dst, dst_ref=dst, send_sem=ssem.at[0], recv_sem=rsem.at[recv],
            device_id=partner, device_id_type=MESH,
        ).wait_recv()

    P1 = [[recv_ids("p1", k, b) for b in range(2)] for k in range(4)]
    ST = [recv_ids("st", i) for i in range(8)]
    P3 = [[recv_ids("p3", k, i) for i in range(2)] for k in range(4)]
    P1T = [[recv_ids("p1t", k, b) for b in range(2)] for k in range(4)]
    P3T = [[recv_ids("p3t", k, i) for i in range(2)] for k in range(4)]

    barrier = pltpu.get_barrier_semaphore()
    greeted = [up, dn, far, partner]
    for k in range(4):
        greeted += dests[k] + sources[k]
    for dev in greeted:
        pl.semaphore_signal(barrier, inc=1, device_id=dev, device_id_type=MESH)

    wcopies = []
    for n in range(NT):
        cols = pl.ds(n * 128, 128)
        wcopies.append([
            pltpu.make_async_copy(wg_ref.at[:, cols], wgu.at[n, :, pl.ds(0, 128)], wsem.at[2 * n]),
            pltpu.make_async_copy(wu_ref.at[:, cols], wgu.at[n, :, pl.ds(128, 128)], wsem.at[2 * n + 1]),
        ])
    dcopy = pltpu.make_async_copy(wd_ref, wdn, wsem.at[2 * NT])
    for pair in wcopies:
        for copy in pair:
            copy.start()
    dcopy.start()

    meta2[0:128, :] = meta_ref[...]
    tok2[0:128, :] = tok_ref[...]
    pl.semaphore_wait(barrier, len(greeted))

    send(("meta",), meta_ref, meta2.at[pl.ds(128, 128)], partner, recv_ids("meta"))
    send(("tok",), tok_ref, tok2.at[pl.ds(128, 128)], partner, recv_ids("tok"))
    tcols = pl.ds(WS, WT)
    scols = pl.ds(0, WS)
    mine, theirs = pl.ds(0, 128), pl.ds(128, 128)
    for r in (1, 3, 2):
        send(("ty", r), tok_ref.at[:, tcols], tokT.at[4 - r, mine], round_y[r], recv_ids("ty", 4 - r))

    rid = lax.broadcasted_iota(jnp.int32, (256, 256), 0)
    cid = lax.broadcasted_iota(jnp.int32, (256, 256), 1)
    lower = jnp.where((rid // 64 == cid // 64) & (rid > cid), 1.0, 0.0).astype(BF16)
    arrived(meta2.at[pl.ds(128, 128)], recv_ids("meta"))
    meta = meta2[...]
    lane = lax.broadcasted_iota(jnp.int32, (256, 128), 1).astype(F32)
    r0, r1 = meta[:, 8:9], meta[:, 9:10]
    oh0 = jnp.where(lane == r0, 1.0, 0.0)
    oh1 = jnp.where(lane == r1, 1.0, 0.0)
    both = oh0 + oh1
    before = jnp.dot(lower, both.astype(BF16), preferred_element_type=F32)
    place0 = jnp.sum(before * oh0, axis=1, keepdims=True)
    place1 = jnp.sum(before * oh1, axis=1, keepdims=True)
    p0 = jnp.sum(meta * oh0, axis=1, keepdims=True)
    p1 = jnp.sum(meta * oh1, axis=1, keepdims=True)
    w0 = p0 / (p0 + p1)
    w1 = p1 / (p0 + p1)
    base = ((lax.broadcasted_iota(jnp.int32, (256, 1), 0) // 64) * CAP).astype(F32)
    s0 = base + place0
    s1 = base + place1

    def columns(k):
        e = (2 * ((x + 4 - SHIFTS[k]) % 4) + c).astype(F32)
        return jnp.where(r0 == e, s0, -1.0), jnp.where(r1 == e, s1, -1.0)

    def two_rows(v):
        a = jnp.sum(v[0:64] , axis=0, keepdims=True) + jnp.sum(v[128:192], axis=0, keepdims=True)
        b = jnp.sum(v[64:128], axis=0, keepdims=True) + jnp.sum(v[192:256], axis=0, keepdims=True)
        return a, b

    ca, cb = two_rows(both)
    pa, pb = two_rows(meta)
    stat_out[...] = jnp.concatenate([ca, cb, pa, pb, jnp.zeros((4, 128), F32)], axis=0)

    arrived(tok2.at[pl.ds(128, 128)], recv_ids("tok"))
    slot_lane = lax.broadcasted_iota(jnp.int32, (256, ROWS), 1).astype(F32)
    block = pl.ds(pl.multiple_of(zb * ROWS, 16), ROWS)

    def slots(k, rows):
        return lax.dot_general(
            PL[k], rows, (((0,), (0,)), ((), ())), preferred_element_type=F32
        ).astype(BF16)

    def dispatch(k):
        c0, c1 = columns(k)
        PL[k] = (jnp.where(slot_lane == c0, 1.0, 0.0) + jnp.where(slot_lane == c1, 1.0, 0.0)).astype(BF16)
        S[k] = slots(k, tok2[:, 0:WS])
        for i in range(2):
            send(("p1", k, i), S.at[k], X.at[k, 0, block, scols], dests[k][i], P1[k][0] + zb)

    def tokens_along_y():
        for r in (1, 3, 2):
            arrived(tokT.at[r, mine], recv_ids("ty", r))
            send(("td", r), tokT.at[r, mine], tokT.at[r, theirs], partner, recv_ids("td", r))
        for r in (1, 3, 2):
            arrived(tokT.at[r, theirs], recv_ids("td", r))

    def dispatch_direct(k):
        TS[k, 0] = slots(k, tok2[:, WS:QUART])
        for r in range(1, 4):
            TS[k, r] = slots(k, tokT[r])
        for i in range(2):
            send(("p1t", k, i), TS.at[k], X.at[k, :, block, tcols], dests[k][i], P1T[k][0] + zb)

    def dispatch_stats():
        for k in range(4):
            for i in range(2):
                send(("st", k, i), stat_out, stat_in.at[x * 2 + zb], dests[k][i], ST[0] + x * 2 + zb)

    own = lambda b: pl.ds(b * ROWS, ROWS)
    other = lambda b: pl.ds(HALF + b * ROWS, ROWS)

    def to_partner(k, r, b):
        send(("d", k, r, b), X.at[k, r, own(b), scols], X.at[k, r, other(b), scols], partner,
             recv_ids("d", k, r, b))

    def gather_start(k):
        for b in range(2):
            arrived(X.at[k, 0, own(b), scols], P1[k][b])
            send(("u", k, b), X.at[k, 0, own(b), scols], X.at[k, 3, own(b), scols], up, recv_ids("u", k, b))
            send(("n", k, b), X.at[k, 0, own(b), scols], X.at[k, 1, own(b), scols], dn, recv_ids("n", k, b))
            to_partner(k, 0, b)

    def gather_forward(k):
        arrived(X.at[k, 3, own(0), scols], recv_ids("u", k, 0))
        send(("fu", k), X.at[k, 3, own(0), scols], X.at[k, 2, own(0), scols], up, recv_ids("fu", k))
        to_partner(k, 3, 0)
        arrived(X.at[k, 1, own(0), scols], recv_ids("n", k, 0))
        to_partner(k, 1, 0)
        arrived(X.at[k, 1, own(1), scols], recv_ids("n", k, 1))
        send(("fn", k), X.at[k, 1, own(1), scols], X.at[k, 2, own(1), scols], dn, recv_ids("fn", k))
        to_partner(k, 1, 1)
        arrived(X.at[k, 3, own(1), scols], recv_ids("u", k, 1))
        to_partner(k, 3, 1)

    def gather_direct(k):
        for b in range(2):
            arrived(X.at[k, :, own(b), tcols], P1T[k][b])
            send(("dt", k, b), X.at[k, :, own(b), tcols], X.at[k, :, other(b), tcols], partner,
                 recv_ids("dt", k, b))

    def gather_end(k):
        arrived(X.at[k, 2, own(0), scols], recv_ids("fu", k))
        to_partner(k, 2, 0)
        arrived(X.at[k, 2, own(1), scols], recv_ids("fn", k))
        to_partner(k, 2, 1)
        gather_direct(k)

    def gathered(k):
        for r in (0, 3, 1, 2):
            for b in range(2):
                arrived(X.at[k, r, other(b), scols], recv_ids("d", k, r, b))
        for b in range(2):
            arrived(X.at[k, :, other(b), tcols], recv_ids("dt", k, b))

    def hidden(k, start, stop):
        def tile(n):
            total = None
            for r in range(4):
                rows = pl.ds(pl.multiple_of(((y + r) % 4) * QUART, QUART), QUART)
                term = jnp.dot(X[k, r], wgu[n, rows, :], preferred_element_type=F32)
                total = term if total is None else total + term
            gate, up_ = total[:, :128], total[:, 128:]
            value = gate / (1.0 + jnp.exp(-gate)) * up_
            first = n * 128 if isinstance(n, int) else pl.multiple_of(n * 128, 128)
            H[:, pl.ds(first, 128)] = value.astype(BF16)

        def step(i, carry):
            tile(start + 2 * i)
            tile(start + 2 * i + 1)
            return carry

        if k == 0:
            for n in range(start, stop):
                for copy in wcopies[n]:
                    copy.wait()
        lax.fori_loop(0, (stop - start) // 2, step, 0)
        if (stop - start) % 2:
            tile(stop - 1)

    def down(k, between=None):
        slot = k % 2
        if k == 0:
            dcopy.wait()
        for r in range(4):
            sent("ds", k - 2, r)

        def quarter(r):
            cols = pl.ds(pl.multiple_of(((y + r) % 4) * QUART, QUART), QUART)
            part = jnp.dot(H[...], wdn[:, cols], preferred_element_type=F32)
            OWN[slot, r] = part[:HALF]
            DS[slot, r] = part[HALF:].astype(BF16)

        def share(r):
            send(("ds", k, r), DS.at[slot, r], DR.at[k, r], partner, recv_ids("ds", k, r))

        def step(i, carry):
            quarter(2 + i)
            quarter(1 - i)
            return carry

        if k < 3:
            lax.fori_loop(0, 2, step, 0)
            for r in (2, 1, 3, 0):
                share(r)
        else:
            for r in (2, 1, 3, 0):
                quarter(r)
                share(r)
                if r == 1:
                    between()

    shared = set()

    def chip_sum(k, r, a, b):
        if (k, r) not in shared:
            shared.add((k, r))
            arrived(DR.at[k, r], recv_ids("ds", k, r))
        return OWN[k % 2, r, :, a:b] + DR[k, r, :, a:b].astype(F32)

    def scatter_start(k):
        slot = k % 2
        sent("a1", k - 2)
        sent("b1", k - 2)
        T1[slot] = chip_sum(k, 2, 0, WS).astype(BF16)
        send(("a1", k), T1.at[slot, pl.ds(0, ROWS)], RR1.at[k, 0], dn, recv_ids("a1", k))
        send(("b1", k), T1.at[slot, pl.ds(ROWS, ROWS)], RR1.at[k, 1], up, recv_ids("b1", k))

    def return_direct(k):
        slot = k % 2
        for b in range(2):
            sent("p3t", k - 2, b)
        for r in (2, 1, 3, 0):
            T4[slot, r] = chip_sum(k, r, WS, QUART).astype(BF16)
        for b in range(2):
            send(("p3t", k, b), T4.at[slot, :, own(b)], RT.at[k, :, block], sources[k][b], P3T[k][0] + zb)

    def scatter_forward(k):
        slot = k % 2
        sent("a2", k - 2)
        sent("b2", k - 2)
        total = chip_sum(k, 3, 0, WS)
        arrived(RR1.at[k, 0], recv_ids("a1", k))
        T2[slot, 0, 0:ROWS] = (total[:ROWS] + RR1[k, 0].astype(F32)).astype(BF16)
        T2[slot, 0, ROWS:HALF] = total[ROWS:].astype(BF16)
        send(("a2", k), T2.at[slot, 0], RR2.at[k, 0], dn, recv_ids("a2", k))
        total = chip_sum(k, 1, 0, WS)
        arrived(RR1.at[k, 1], recv_ids("b1", k))
        T2[slot, 1, 0:ROWS] = total[:ROWS].astype(BF16)
        T2[slot, 1, ROWS:HALF] = (total[ROWS:] + RR1[k, 1].astype(F32)).astype(BF16)
        send(("b2", k), T2.at[slot, 1], RR2.at[k, 1], up, recv_ids("b2", k))

    def scatter_end(k):
        slot = k % 2
        for b in range(2):
            sent("p3", k - 2, b)
        total = chip_sum(k, 0, 0, WS)
        arrived(RR2.at[k, 0], recv_ids("a2", k))
        arrived(RR2.at[k, 1], recv_ids("b2", k))
        T3[slot] = (total + RR2[k, 0].astype(F32) + RR2[k, 1].astype(F32)).astype(BF16)
        for b in range(2):
            send(("p3", k, b), T3.at[slot, own(b)], R.at[k, block], sources[k][b], P3[k][0] + zb)

    two_lane = lax.broadcasted_iota(jnp.int32, (256, HALF), 1)
    two_lane = jnp.where(two_lane >= ROWS, two_lane - ROWS, two_lane).astype(F32)

    def weights(k):
        c0, c1 = columns(k)
        weight = jnp.where(two_lane == c0, w0, 0.0) + jnp.where(two_lane == c1, w1, 0.0)
        high = weight.astype(BF16)
        return high, (weight - high.astype(F32)).astype(BF16)

    def mix(high, low, rows):
        return jnp.dot(high, rows, preferred_element_type=F32) + jnp.dot(
            low, rows, preferred_element_type=F32
        )

    def combine_direct(k):
        for i in range(2):
            arrived(RT.at[k, :, own(i)], P3T[k][i])
        high, low = weights(k)
        for r in range(4):
            term = mix(high, low, RT[k, r])
            accT[r] = term if k == 0 else accT[r] + term

    def combine(k):
        for i in range(2):
            arrived(R.at[k, own(i)], P3[k][i])
        high, low = weights(k)
        term = mix(high, low, R[k])
        acc[...] = term if k == 0 else acc[...] + term

    dispatch(0)
    dispatch(1)
    tokens_along_y()
    dispatch_direct(0)
    gather_start(0)
    dispatch(2)
    dispatch(3)
    dispatch_direct(1)
    gather_start(1)
    gather_forward(0)
    gather_start(2)
    dispatch_stats()
    gather_end(0)
    gather_forward(1)
    gathered(0)

    hidden(0, 0, 3)
    dispatch_direct(2)
    gather_start(3)
    hidden(0, 3, NT)
    dispatch_direct(3)
    gather_end(1)
    gather_forward(2)
    for i in range(8):
        arrived(stat_in.at[i], ST[i])
    total = stat_in[0]
    for i in range(1, 8):
        total = total + stat_in[i]
    stat_pair[0] = total
    send(("sp",), stat_pair.at[0], stat_pair.at[1], partner, recv_ids("sp"))
    down(0)
    gather_forward(3)
    gathered(1)

    hidden(1, 0, 3)
    scatter_start(0)
    return_direct(0)
    gather_end(2)
    hidden(1, 3, NT)
    scatter_forward(0)
    gather_end(3)
    down(1)
    gathered(2)

    hidden(2, 0, 3)
    scatter_start(1)
    return_direct(1)
    scatter_end(0)
    hidden(2, 3, NT)
    scatter_forward(1)
    down(2)
    gathered(3)

    hidden(3, 0, 3)
    scatter_start(2)
    return_direct(2)
    scatter_end(1)
    combine_direct(0)
    hidden(3, 3, NT)
    scatter_forward(2)
    combine(0)
    combine_direct(1)
    down(3, lambda: scatter_start(3))
    scatter_end(2)
    scatter_forward(3)
    return_direct(3)
    combine_direct(2)
    combine(1)
    combine_direct(3)
    send(("finT",), accT.at[:, theirs], finT_in, partner, recv_ids("finT"))
    arrived(stat_pair.at[1], recv_ids("sp"))
    total = stat_pair[0] + stat_pair[1]
    aux_ref[...] = EXPERTS * (total[0:2, 0:8] / 4096.0) * (total[2:4, 0:8] / 2048.0)
    combine(2)
    arrived(finT_in, recv_ids("finT"))
    for r in (2, 1, 3):
        YS[r] = (accT[r, 0:128] + finT_in[r]).astype(BF16)
        send(("ys", r), YS.at[r], YR.at[r], round_y[r], recv_ids("ys", r))
    scatter_end(3)
    combine(3)
    send(("fin",), acc.at[theirs], fin_in, partner, recv_ids("fin"))
    total = accT[0, 0:128] + finT_in[0]
    for r in (1, 3, 2):
        arrived(YR.at[r], recv_ids("ys", r))
        total = total + YR[r].astype(F32)
    out_ref[:, WS:QUART] = total.astype(BF16)
    arrived(fin_in, recv_ids("fin"))
    out_ref[:, 0:WS] = (acc[0:128, :] + fin_in[...]).astype(BF16)
    for name in list(pending):
        sent(*name)
    assert len(send_ids.names) <= N_SEND and len(recv_ids.names) <= N_RECV


def local(tokens, routes, probs, w_gate, w_up, w_down):
    meta = jnp.concatenate(
        [probs.reshape(128, EXPERTS), routes.reshape(128, 2).astype(F32), jnp.zeros((128, 118), F32)], axis=1
    )
    vmem = pl.BlockSpec(memory_space=pltpu.VMEM)
    hbm = pl.BlockSpec(memory_space=pl.ANY)
    mixed, aux = pl.pallas_call(
        moe_kernel,
        out_shape=(jax.ShapeDtypeStruct((128, QUART), BF16), jax.ShapeDtypeStruct((2, 8), F32)),
        in_specs=[vmem, vmem, hbm, hbm, hbm],
        out_specs=(vmem, vmem),
        scratch_shapes=[
            pltpu.VMEM((NT, D, 256), BF16),
            pltpu.VMEM((FFD, D), BF16),
            pltpu.VMEM((4, 4, FULL, QUART), BF16),
            pltpu.VMEM((FULL, FFD), BF16),
            pltpu.VMEM((4, ROWS, WS), BF16),
            pltpu.VMEM((4, 4, ROWS, WT), BF16),
            pltpu.VMEM((256, QUART), BF16),
            pltpu.VMEM((4, 256, WT), BF16),
            pltpu.VMEM((4, 256, ROWS), BF16),
            pltpu.VMEM((256, 128), F32),
            pltpu.VMEM((256, WS), F32),
            pltpu.VMEM((4, 256, WT), F32),
            pltpu.VMEM((4, HALF, WS), BF16),
            pltpu.VMEM((4, 4, HALF, WT), BF16),
            pltpu.VMEM((2, 4, HALF, QUART), BF16),
            pltpu.VMEM((4, 4, HALF, QUART), BF16),
            pltpu.VMEM((2, 4, HALF, QUART), F32),
            pltpu.VMEM((2, HALF, WS), BF16),
            pltpu.VMEM((2, 2, HALF, WS), BF16),
            pltpu.VMEM((2, HALF, WS), BF16),
            pltpu.VMEM((2, 4, HALF, WT), BF16),
            pltpu.VMEM((4, 2, ROWS, WS), BF16),
            pltpu.VMEM((4, 2, HALF, WS), BF16),
            pltpu.VMEM((128, WS), F32),
            pltpu.VMEM((4, 128, WT), F32),
            pltpu.VMEM((4, 128, WT), BF16),
            pltpu.VMEM((4, 128, WT), BF16),
            pltpu.VMEM((8, 128), F32),
            pltpu.VMEM((8, 8, 128), F32),
            pltpu.VMEM((2, 8, 128), F32),
            pltpu.SemaphoreType.DMA((2 * NT + 1,)),
            pltpu.SemaphoreType.DMA((N_SEND,)),
            pltpu.SemaphoreType.DMA((N_RECV,)),
        ],
        compiler_params=pltpu.CompilerParams(
            collective_id=0, has_side_effects=True, vmem_limit_bytes=66_000_000
        ),
        name="moe",
    )(tokens.reshape(128, QUART), meta, w_gate[0], w_up[0], w_down[0])
    return mixed.reshape(MICRO, 64, QUART), aux


def solution(mesh):
    in_specs = (
        P(None, "dp", "tensor"),
        P(None, "dp", None),
        P(None, "dp", None),
        P("dp", None, "tensor"),
        P("dp", None, "tensor"),
        P("dp", "tensor", None),
    )
    out_specs = (P(None, "dp", "tensor"), P())
    return jax.shard_map(local, mesh=mesh, in_specs=in_specs, out_specs=out_specs, check_vma=False)
```
